32 devices in a mesh: img: 2 (over x), neu: 16 (over z, y, core).
Axes of the slice: x: 2, y: 2, z: 4, core: 2. Of those that a mesh axis runs over, the one named last changes fastest.
Arguments:
- image_values: bfloat16 [4096, 1024], P('neu', 'img'), may hold values from 0.25 to 16
- image_mask: int32 [4096, 1024], P('neu', 'img'), may hold values 0 or 1
- weights: bfloat16 [3, 4096, 4, 8], P(None, 'neu'), may hold values from -0.25 to 0.34960938
- block_index: int32 [3, 128, 4], P(None, 'neu'), may hold values from 0 to 511, as said below
Outputs:
- activations: bfloat16 [4096, 1024], P('neu', 'img')
- row_sums: float32 [1024], P(('img', 'neu'))
The draws below stay inside these ranges and needn't reach their ends.
Inputs may be any that keep to these rules, and one draw needn't show every extreme that they name: Split the 512 input blocks into 16 runs of consecutive blocks, and the 128 output blocks likewise; if output block b lies in run s, block_index[l, b, k] lies in run (s + k * 4 + l) mod 16.
All inputs are finite; a program needn't handle non-finite values. No bound on the sum of `image_mask` on one device may be relied on, other than what follows from the above.
Results may differ from the reference program's by a relative error of at most 0.0035.
Values may be sent and summed in bfloat16 or wider, within the bound.
A program may use at most 64 MiB of HBM per device.

```python
import math
import jax
import jax.numpy as jnp

NEU = 4096
LAYERS = 3
KB = 4
IB = 8
OB = 32
IMAGES = 1024
NOB = 128
N_NEU = 16


def draw_block_index(key, part):
    per_run = NEU // IB // N_NEU
    outs_per_run = NOB // N_NEU
    owner = jnp.arange(NOB, dtype=jnp.int32) // outs_per_run
    layer_ids = jnp.arange(LAYERS, dtype=jnp.int32)
    slot_ids = jnp.arange(KB, dtype=jnp.int32)
    source = (owner[None, :, None] + slot_ids[None, None, :] * (N_NEU // KB) + layer_ids[:, None, None]) % N_NEU
    inner = jax.random.randint(jax.random.fold_in(key, 7), (LAYERS, NOB, KB), 0, per_run, dtype=jnp.int32)
    return (source * per_run + inner).astype(jnp.int32)


def place_ends(values, stream_key, low, high):
    extent = values.shape
    index_at = [jax.random.randint(jax.random.fold_in(stream_key, axis), (), 0, extent[axis]) for axis in range(len(extent))]
    values = values.at[tuple(index_at)].set(low)
    longest = extent.index(max(extent))
    index_at[longest] = (index_at[longest] + 1) % extent[longest]
    return values.at[tuple(index_at)].set(high)


def block_scale(stream_key, extent, pieces, least, high):
    factor_of, own = 1.0, jax.random.fold_in(stream_key, 6)
    for dim, blocks in pieces:
        draws = jnp.exp(jax.random.uniform(jax.random.fold_in(own, dim), (blocks,), jnp.float32, least / len(pieces), high / len(pieces)))
        factor_of = factor_of * jnp.repeat(draws, extent[dim] // blocks).reshape([-1 if axis == dim else 1 for axis in range(len(extent))])
    return factor_of


def setup_inputs(seed: int = 0) -> dict:
    splits = jax.random.split(jax.random.key(seed), 5)
    return {
        "image_values": jnp.clip(jnp.exp(math.log(16.0) - 4.158883 * jax.random.uniform(splits[0], (NEU, IMAGES), jnp.float32) ** block_scale(splits[0], (NEU, IMAGES), ((0, 16), (1, 2)), -0.2, 0.2)), 0.25, 16.0).astype(jnp.bfloat16),
        "image_mask": place_ends((jax.random.randint(splits[1], (NEU, IMAGES), 0, 2) < 1).astype(jnp.int32), jax.random.fold_in(splits[1], 1), 0, 1),
        "weights": jnp.clip(-0.25 + 0.5996094 * jax.random.uniform(splits[2], (LAYERS, NEU, KB, IB), jnp.float32) ** block_scale(splits[2], (LAYERS, NEU, KB, IB), ((1, 16),), -0.2, 0.2), -0.25, 0.34960938).astype(jnp.bfloat16),
        "block_index": draw_block_index(jax.random.fold_in(splits[4], 71), 0),
    }


bias_value = 0.35
ceiling = 32.0


def advance(activity, layer_weights, layer_blocks):
    offsets = jnp.arange(IB, dtype=jnp.int32)
    rows_wanted = (layer_blocks.astype(jnp.int32)[:, :, None] * IB + offsets[None, None, :]).reshape(-1)
    picked = jnp.take(activity, rows_wanted, axis=0).reshape(layer_blocks.shape[0], KB * IB, -1).astype(jnp.float32)
    weights_full = layer_weights.reshape(layer_blocks.shape[0], OB, KB * IB).astype(jnp.float32)
    summed = jnp.einsum("dom,dmr->dor", weights_full, picked)
    clamped = jnp.minimum(jnp.maximum(summed - bias_value, 0.0), ceiling)
    return clamped.astype(jnp.bfloat16).reshape(NEU, -1)


def reference(image_values, image_mask, weights, block_index):
    activity = image_values * image_mask.astype(jnp.bfloat16)
    for layer_number in range(LAYERS):
        activity = advance(activity, weights[layer_number], block_index[layer_number])
    totals = jnp.sum(activity.astype(jnp.float32), axis=0)
    return activity, totals
```

```python
import functools

import jax
import jax.numpy as jnp
from jax import lax
from jax.experimental import pallas as pl
from jax.experimental.pallas import tpu as pltpu
from jax.sharding import PartitionSpec as P

KB = 4
IB = 8
OB = 32

bias_value = 0.35
ceiling = 32.0


def quotient(x, n):
    return x >> (n.bit_length() - 1) if n & (n - 1) == 0 else lax.div(x, jnp.int32(n))


def remainder(x, n):
    return x & (n - 1) if n & (n - 1) == 0 else lax.rem(x, jnp.int32(n))


def kernel(
    geometry, val_hbm, mask_hbm, wt_hbm, idx_hbm, out_ref, rs_ref,
    val, mask, y0, xin, ya, yb, wt, wd, idx_v, idx_s, tiles, part, parts,
    load_sem, in_send, in_recv, w_send, w_recv, i_send, i_recv, s_sem, o_send, o_recv, r_send, r_recv,
):
    classes, layers, rows, blocks, lanes = geometry
    group = KB
    devices = classes * group
    shift = [l * (l + 1) // 2 for l in range(layers)]
    me = lax.axis_index("neu")
    q, c = me // classes, me % classes
    run_blocks = rows // IB

    def device(dq, dc):
        return ((q + dq) % group) * classes + (c + dc) % classes

    def remote(src, dst, send, recv, dq, dc):
        return pltpu.make_async_remote_copy(
            src_ref=src, dst_ref=dst, send_sem=send, recv_sem=recv,
            device_id={"neu": device(dq, dc)}, device_id_type=pl.DeviceIdType.MESH,
        )

    order = [d for d in (2, 1, 3)]

    loads = []
    for n, d in enumerate(order + [0]):
        t = (q + d) % group
        cols = pl.ds(pl.multiple_of(t * lanes, lanes), lanes)
        a = pltpu.make_async_copy(val_hbm.at[:, cols], val.at[d], load_sem.at[0, d])
        b = pltpu.make_async_copy(mask_hbm.at[:, cols], mask.at[d], load_sem.at[1, d])
        a.start()
        b.start()
        loads.append((d, a, b))

    partners = set()
    for dq in range(group):
        for s in shift:
            partners |= {(dq, s % classes), (dq, -s % classes)}
    for dc in range(classes):
        partners.add((0, dc))
    partners.discard((0, 0))
    barrier = pltpu.get_barrier_semaphore()
    for dq, dc in sorted(partners):
        pl.semaphore_signal(
            barrier, inc=1, device_id={"neu": device(dq, dc)},
            device_id_type=pl.DeviceIdType.MESH,
        )
    pl.semaphore_wait(barrier, len(partners))

    waits = []

    def send_weights(l):
        pending = []
        for dq in order + [0]:
            if dq == 0 and shift[l] % classes == 0:
                a = pltpu.make_async_copy(wt_hbm.at[l], wt.at[l, q], w_recv.at[l, 0])
                b = pltpu.make_async_copy(idx_hbm.at[l], idx_v.at[l, q], i_recv.at[l, 0])
                a.start()
                b.start()
                pending += [(a.wait, b.wait)]
                continue
            b = remote(idx_hbm.at[l], idx_v.at[l, q], i_send.at[l, dq], i_recv.at[l, dq], dq, shift[l])
            a = remote(wt_hbm.at[l], wt.at[l, q], w_send.at[l, dq], w_recv.at[l, dq], dq, shift[l])
            b.start()
            a.start()
            waits.extend([a.wait_send, b.wait_send])
            pending += [(a.wait_recv, b.wait_recv)]
        return pending

    pending_w = [None] * layers
    pending_w[0] = send_weights(0)

    inputs = []
    for d, a, b in loads:
        a.wait()
        b.wait()
        masked = (val[d].astype(jnp.float32) * mask[d].astype(jnp.float32))
        if d:
            y0[d] = masked.astype(jnp.bfloat16)
            x = remote(y0.at[d], xin.at[d], in_send.at[d], in_recv.at[d], d, 0)
            x.start()
            waits.append(x.wait_send)
            inputs.append((d, x))
        else:
            ya[pl.ds(q * run_blocks, run_blocks)] = masked.reshape(run_blocks, IB, lanes)
    for l in range(1, layers):
        pending_w[l] = send_weights(l)

    per = min(4, blocks)
    width = per * OB
    m_of = lax.broadcasted_iota(jnp.int32, (width, width), 0) // (KB * IB)
    n_of = lax.broadcasted_iota(jnp.int32, (width, width), 1) // OB

    def prepare(l):
        for a, b in pending_w[l]:
            b()
        c0 = pltpu.make_async_copy(idx_v.at[l], idx_s.at[l], s_sem.at[l])
        c0.start()
        for a, b in pending_w[l]:
            a()
        for t in range(group):
            for g in range(blocks // per):
                w = wt[l, t, :, g * width:(g + 1) * width].astype(jnp.float32)
                wide = jnp.where(m_of == n_of, jnp.concatenate([w] * per, axis=0), 0.0)
                wd[l, t, g] = wide.T.astype(jnp.bfloat16)
        c0.wait()

    def advance(l, src, t):
        out = []
        for g in range(blocks // per):
            pieces = []
            for j in range(g * per, (g + 1) * per):
                for k in range(KB):
                    b = idx_s[l, t, k, j]
                    pieces.append(src[quotient(b, run_blocks * classes) * run_blocks + remainder(b, run_blocks)])
            picked = jnp.concatenate(pieces, axis=0).astype(jnp.bfloat16)
            summed = jnp.dot(wd[l, t, g], picked, preferred_element_type=jnp.float32)
            clamped = jnp.minimum(jnp.maximum(summed - bias_value, 0.0), ceiling)
            out.append(clamped.astype(jnp.bfloat16))
        return out

    prepare(0)
    for d, x in inputs:
        x.wait_recv()
        s = (q + group - d) % group
        ya[pl.ds(s * run_blocks, run_blocks)] = xin[d].astype(jnp.float32).reshape(run_blocks, IB, lanes)

    src, dst = ya, yb
    for l in range(layers - 1):
        for t in range(group):
            for g, y in enumerate(advance(l, src, t)):
                first = t * run_blocks + g * width // IB
                dst[first:first + width // IB] = y.astype(jnp.float32).reshape(width // IB, IB, lanes)
        prepare(l + 1)
        src, dst = dst, src

    total = jnp.zeros((8, lanes), jnp.float32)
    last = layers - 1
    outputs = []
    for d in order + [0]:
        t = (q + d) % group
        for g, y in enumerate(advance(last, src, t)):
            tiles[d, g * width:(g + 1) * width, :] = y
            total = total + jnp.sum(y.astype(jnp.float32).reshape(width // 8, 8, lanes), axis=0)
        x = remote(
            tiles.at[d], out_ref.at[:, pl.ds(pl.multiple_of(q * lanes, lanes), lanes)],
            o_send.at[d], o_recv.at[d], d, -shift[last],
        )
        x.start()
        waits.append(x.wait_send)
        outputs.append(x)

    part[...] = total
    sums = []
    for dc in range(1, classes):
        x = remote(part, parts.at[dc], r_send.at[dc], r_recv.at[dc], 0, dc)
        x.start()
        waits.append(x.wait_send)
        sums.append((dc, x))
    for dc, x in sums:
        x.wait_recv()
        total = total + parts[dc]
    row = jnp.sum(total, axis=0, keepdims=True)
    share = lanes // classes
    mine = jnp.zeros((1, share), jnp.float32)
    for j in range(classes):
        mine = jnp.where(c == j, row[:, j * share:(j + 1) * share], mine)
    rs_ref[...] = mine
    for x in outputs:
        x.wait_recv()
    for w in waits:
        w()


def on_device(classes, image_values, image_mask, weights, block_index):
    layers, rows = weights.shape[:2]
    blocks = block_index.shape[1]
    columns = image_values.shape[1]
    group = KB
    lanes = columns // group
    wt = jnp.transpose(weights, (0, 2, 3, 1)).reshape(layers, KB * IB, rows)
    idx = jnp.transpose(block_index, (0, 2, 1))
    per = min(4, blocks)
    bf16, f32, i32 = jnp.bfloat16, jnp.float32, jnp.int32
    V, S = pltpu.VMEM, pltpu.SMEM
    dma = pltpu.SemaphoreType.DMA
    any_spec = pl.BlockSpec(memory_space=pl.ANY)
    out, sums = pl.pallas_call(
        functools.partial(kernel, (classes, layers, rows, blocks, lanes)),
        out_shape=(
            jax.ShapeDtypeStruct((rows, columns), bf16),
            jax.ShapeDtypeStruct((1, lanes // classes), f32),
        ),
        in_specs=[any_spec] * 4,
        out_specs=(pl.BlockSpec(memory_space=pltpu.VMEM), pl.BlockSpec(memory_space=pltpu.VMEM)),
        scratch_shapes=[
            V((group, rows, lanes), bf16),
            V((group, rows, lanes), i32),
            V((group, rows, lanes), bf16),
            V((group, rows, lanes), bf16),
            V((group * rows // IB, IB, lanes), f32),
            V((group * rows // IB, IB, lanes), f32),
            V((layers, group, KB * IB, rows), bf16),
            V((layers, group, blocks // per, per * OB, per * KB * IB), bf16),
            V((layers, group, KB, blocks), i32),
            S((layers, group, KB, blocks), i32),
            V((group, rows, lanes), bf16),
            V((8, lanes), f32),
            V((classes, 8, lanes), f32),
            dma((2, group)),
            dma((group,)), dma((group,)),
            dma((layers, group)), dma((layers, group)),
            dma((layers, group)), dma((layers, group)),
            dma((layers,)),
            dma((group,)), dma((group,)),
            dma((classes,)), dma((classes,)),
        ],
        compiler_params=pltpu.CompilerParams(collective_id=0, has_side_effects=True),
    )(image_values, image_mask, wt, idx)
    return out, sums.reshape(-1)


def solution(mesh):
    classes = mesh.shape["neu"] // KB
    in_specs = (P("neu", "img"), P("neu", "img"), P(None, "neu", None, None), P(None, "neu", None))
    out_specs = (P("neu", "img"), P(("img", "neu")))
    return jax.shard_map(
        functools.partial(on_device, classes), mesh=mesh, in_specs=in_specs,
        out_specs=out_specs, check_vma=False,
    )
```

```python
import functools

import jax
import jax.numpy as jnp
from jax import lax
from jax.experimental import pallas as pl
from jax.experimental.pallas import tpu as pltpu
from jax.sharding import PartitionSpec as P

KB = 4
IB = 8
OB = 32

bias_value = 0.35
ceiling = 32.0


def quotient(x, n):
    return x >> (n.bit_length() - 1) if n & (n - 1) == 0 else lax.div(x, jnp.int32(n))


def remainder(x, n):
    return x & (n - 1) if n & (n - 1) == 0 else lax.rem(x, jnp.int32(n))


def kernel(
    geometry, val_hbm, mask_hbm, wt_hbm, idx_hbm, out_ref, rs_ref,
    val, mask, w_src, i_src, y0, xin, ya, yb, wt, wd, idx_v, idx_s, tiles, part, parts,
    load_sem, own_sem, f_send, f_recv, in_send, in_recv, w_send, w_recv, i_send, i_recv, s_sem, o_send, o_recv, r_send, r_recv,
):
    classes, pairs, layers, rows, blocks, lanes = geometry
    group = KB
    devices = classes * group
    shift = [l * (l + 1) // 2 for l in range(layers)]
    me = lax.axis_index("neu")
    q, c = me // classes, me % classes
    run_blocks = rows // IB

    def device(dq, dc):
        return ((q + dq) % group) * classes + (c + dc) % classes

    def remote(src, dst, send, recv, dq, dc):
        return pltpu.make_async_remote_copy(
            src_ref=src, dst_ref=dst, send_sem=send, recv_sem=recv,
            device_id={"neu": device(dq, dc)}, device_id_type=pl.DeviceIdType.MESH,
        )

    order = [d for d in (2, 1, 3)]

    own = [
        pltpu.make_async_copy(wt_hbm, w_src, own_sem.at[0]),
        pltpu.make_async_copy(idx_hbm, i_src, own_sem.at[1]),
    ]
    loads = []
    for d in order + [0]:
        t = (q + d) % group
        cols = pl.ds(pl.multiple_of(t * lanes, lanes), lanes)
        a = pltpu.make_async_copy(val_hbm.at[:, cols], val.at[d], load_sem.at[0, d])
        b = pltpu.make_async_copy(mask_hbm.at[:, cols], mask.at[d], load_sem.at[1, d])
        loads.append((d, a, b))
    for a in own:
        a.start()
    for d, a, b in loads:
        a.start()
        b.start()

    partners = set()
    for dq in range(group):
        for s in shift:
            partners |= {(dq, s % classes), (dq, -s % classes)}
    for dc in range(classes):
        partners.add((0, dc))
    partners.discard((0, 0))
    barrier = pltpu.get_barrier_semaphore()
    for dq, dc in sorted(partners, reverse=True):
        pl.semaphore_signal(
            barrier, inc=1, device_id={"neu": device(dq, dc)},
            device_id_type=pl.DeviceIdType.MESH,
        )
    if pairs:
        x_me = lax.axis_index("img")
        half = x_me % 2
        twin = x_me + 1 - 2 * half
        share_rows = KB * IB // 2
        w_rows = pl.ds(pl.multiple_of(half * share_rows, share_rows), share_rows)
        pl.semaphore_signal(
            barrier, inc=1, device_id={"img": twin}, device_id_type=pl.DeviceIdType.MESH
        )
    else:
        w_rows = pl.ds(0, KB * IB)

    for d, a, b in loads:
        a.wait()
        b.wait()
        masked = (val[d].astype(jnp.float32) * mask[d].astype(jnp.float32))
        if d:
            y0[d] = masked.astype(jnp.bfloat16)
        else:
            ya[pl.ds(q * run_blocks, run_blocks)] = masked.reshape(run_blocks, IB, lanes)
    for a in own:
        a.wait()
    pl.semaphore_wait(barrier, len(partners) + (1 if pairs else 0))

    waits = []
    index_waits = [[] for _ in range(layers)]
    weight_sends = []
    weight_waits = [[] for _ in range(layers)]
    for l in range(layers):
        for dq in order + [0]:
            if dq == 0 and shift[l] % classes == 0:
                a = pltpu.make_async_copy(w_src.at[l], wt.at[l, q], w_recv.at[l, 0])
                b = pltpu.make_async_copy(i_src.at[l], idx_v.at[l, q], i_recv.at[l, 0])
                a.start()
                b.start()
                weight_waits[l].append(a.wait)
                index_waits[l].append(b.wait)
                continue
            b = remote(i_src.at[l], idx_v.at[l, q], i_send.at[l, dq], i_recv.at[l, dq], dq, shift[l])
            a = remote(
                w_src.at[l, w_rows], wt.at[l, q, w_rows], w_send.at[l, dq], w_recv.at[l, dq], dq, shift[l]
            )
            b.start()
            a.start()
            waits.extend([a.wait_send, b.wait_send])
            index_waits[l].append(b.wait_recv)
            weight_sends.append((l, dq, a))

    inputs = []
    for d in order:
        x = remote(y0.at[d], xin.at[d], in_send.at[d], in_recv.at[d], d, 0)
        x.start()
        waits.append(x.wait_send)
        inputs.append((d, x))

    for l, dq, a in weight_sends:
        a.wait_recv()
        if pairs:
            here = wt.at[l, (q + group - dq) % group, w_rows]
            x = pltpu.make_async_remote_copy(
                src_ref=here, dst_ref=here, send_sem=f_send.at[l, dq], recv_sem=f_recv.at[l, dq],
                device_id={"img": twin}, device_id_type=pl.DeviceIdType.MESH,
            )
            x.start()
            waits.append(x.wait_send)
            weight_waits[l].append(x.wait_recv)

    index_copies = []
    for l in range(layers):
        for w in index_waits[l]:
            w()
        x = pltpu.make_async_copy(idx_v.at[l], idx_s.at[l], s_sem.at[l])
        x.start()
        index_copies.append(x)

    per = min(4, blocks)
    width = per * OB
    m_of = lax.broadcasted_iota(jnp.int32, (width, width), 0) // (KB * IB)
    n_of = lax.broadcasted_iota(jnp.int32, (width, width), 1) // OB

    def prepare(l):
        for w in weight_waits[l]:
            w()
        for t in range(group):
            for g in range(blocks // per):
                w = wt[l, t, :, g * width:(g + 1) * width].astype(jnp.float32)
                wide = jnp.where(m_of == n_of, jnp.concatenate([w] * per, axis=0), 0.0)
                wd[l, t, g] = wide.T.astype(jnp.bfloat16)

    def advance(l, src, t):
        out = []
        for g in range(blocks // per):
            pieces = []
            for j in range(g * per, (g + 1) * per):
                for k in range(KB):
                    b = idx_s[l, t, k, j]
                    pieces.append(src[quotient(b, run_blocks * classes) * run_blocks + remainder(b, run_blocks)])
            picked = jnp.concatenate(pieces, axis=0).astype(jnp.bfloat16)
            summed = jnp.dot(wd[l, t, g], picked, preferred_element_type=jnp.float32)
            clamped = jnp.minimum(jnp.maximum(summed - bias_value, 0.0), ceiling)
            out.append(clamped.astype(jnp.bfloat16))
        return out

    for l in range(layers):
        prepare(l)
    for x in index_copies:
        x.wait()
    for d, x in inputs:
        x.wait_recv()
        s = (q + group - d) % group
        ya[pl.ds(s * run_blocks, run_blocks)] = xin[d].astype(jnp.float32).reshape(run_blocks, IB, lanes)

    src, dst = ya, yb
    for l in range(layers - 1):
        for t in range(group):
            for g, y in enumerate(advance(l, src, t)):
                first = t * run_blocks + g * width // IB
                dst[first:first + width // IB] = y.astype(jnp.float32).reshape(width // IB, IB, lanes)
        src, dst = dst, src

    total = jnp.zeros((8, lanes), jnp.float32)
    last = layers - 1
    outputs = []
    for d in order + [0]:
        t = (q + d) % group
        for g, y in enumerate(advance(last, src, t)):
            tiles[d, g * width:(g + 1) * width, :] = y
            total = total + jnp.sum(y.astype(jnp.float32).reshape(width // 8, 8, lanes), axis=0)
        x = remote(
            tiles.at[d], out_ref.at[:, pl.ds(pl.multiple_of(q * lanes, lanes), lanes)],
            o_send.at[d], o_recv.at[d], d, -shift[last],
        )
        x.start()
        waits.append(x.wait_send)
        outputs.append(x)

    part[...] = total
    sums = []
    for dc in range(1, classes):
        x = remote(part, parts.at[dc], r_send.at[dc], r_recv.at[dc], 0, dc)
        x.start()
        waits.append(x.wait_send)
        sums.append((dc, x))
    for dc, x in sums:
        x.wait_recv()
        total = total + parts[dc]
    row = jnp.sum(total, axis=0, keepdims=True)
    share = lanes // classes
    mine = jnp.zeros((1, share), jnp.float32)
    for j in range(classes):
        mine = jnp.where(c == j, row[:, j * share:(j + 1) * share], mine)
    rs_ref[...] = mine
    for x in outputs:
        x.wait_recv()
    for w in waits:
        w()


def on_device(classes, pairs, image_values, image_mask, weights, block_index):
    layers, rows = weights.shape[:2]
    blocks = block_index.shape[1]
    columns = image_values.shape[1]
    group = KB
    lanes = columns // group
    wt = jnp.transpose(weights, (0, 2, 3, 1)).reshape(layers, KB * IB, rows)
    idx = jnp.transpose(block_index, (0, 2, 1))
    per = min(4, blocks)
    bf16, f32, i32 = jnp.bfloat16, jnp.float32, jnp.int32
    V, S = pltpu.VMEM, pltpu.SMEM
    dma = pltpu.SemaphoreType.DMA
    any_spec = pl.BlockSpec(memory_space=pl.ANY)
    operands = [pltpu.with_memory_space_constraint(v, pltpu.HBM) for v in (image_values, image_mask, wt, idx)]
    out, sums = pl.pallas_call(
        functools.partial(kernel, (classes, pairs, layers, rows, blocks, lanes)),
        out_shape=(
            jax.ShapeDtypeStruct((rows, columns), bf16),
            jax.ShapeDtypeStruct((1, lanes // classes), f32),
        ),
        in_specs=[any_spec] * 4,
        out_specs=(pl.BlockSpec(memory_space=pltpu.VMEM), pl.BlockSpec(memory_space=pltpu.VMEM)),
        scratch_shapes=[
            V((group, rows, lanes), bf16),
            V((group, rows, lanes), i32),
            V((layers, KB * IB, rows), bf16),
            V((layers, KB, blocks), i32),
            V((group, rows, lanes), bf16),
            V((group, rows, lanes), bf16),
            V((group * rows // IB, IB, lanes), f32),
            V((group * rows // IB, IB, lanes), f32),
            V((layers, group, KB * IB, rows), bf16),
            V((layers, group, blocks // per, per * OB, per * KB * IB), bf16),
            V((layers, group, KB, blocks), i32),
            S((layers, group, KB, blocks), i32),
            V((group, rows, lanes), bf16),
            V((8, lanes), f32),
            V((classes, 8, lanes), f32),
            dma((2, group)), dma((2,)),
            dma((layers, group)), dma((layers, group)),
            dma((group,)), dma((group,)),
            dma((layers, group)), dma((layers, group)),
            dma((layers, group)), dma((layers, group)),
            dma((layers,)),
            dma((group,)), dma((group,)),
            dma((classes,)), dma((classes,)),
        ],
        compiler_params=pltpu.CompilerParams(collective_id=0, has_side_effects=True, vmem_limit_bytes=16 * 1024 * 1024),
    )(*operands)
    return out, sums.reshape(-1)


def solution(mesh):
    classes = mesh.shape["neu"] // KB
    in_specs = (P("neu", "img"), P("neu", "img"), P(None, "neu", None, None), P(None, "neu", None))
    out_specs = (P("neu", "img"), P(("img", "neu")))
    return jax.shard_map(
        functools.partial(on_device, classes, mesh.shape["img"] % 2 == 0), mesh=mesh, in_specs=in_specs,
        out_specs=out_specs, check_vma=False,
    )
```

```python
import functools

import jax
import jax.numpy as jnp
from jax import lax
from jax.experimental import pallas as pl
from jax.experimental.pallas import tpu as pltpu
from jax.sharding import PartitionSpec as P

KB = 4
IB = 8
OB = 32

bias_value = 0.35
ceiling = 32.0


def quotient(x, n):
    return x >> (n.bit_length() - 1) if n & (n - 1) == 0 else lax.div(x, jnp.int32(n))


def remainder(x, n):
    return x & (n - 1) if n & (n - 1) == 0 else lax.rem(x, jnp.int32(n))


def kernel(
    geometry, val_hbm, mask_hbm, wt_hbm, idx_hbm, out_ref, rs_ref,
    val, mask, w_src, i_src, y0, xin, ya, yb, wt, wd, idx_v, idx_s, tiles, part, parts,
    load_sem, own_sem, f_send, f_recv, in_send, in_recv, w_send, w_recv, i_send, i_recv, s_sem, o_send, o_recv, r_send, r_recv,
):
    classes, pairs, layers, rows, blocks, lanes = geometry
    group = KB
    devices = classes * group
    shift = [l * (l + 1) // 2 for l in range(layers)]
    me = lax.axis_index("neu")
    q, c = me // classes, me % classes
    run_blocks = rows // IB

    def device(dq, dc):
        return ((q + dq) % group) * classes + (c + dc) % classes

    def remote(src, dst, send, recv, dq, dc):
        return pltpu.make_async_remote_copy(
            src_ref=src, dst_ref=dst, send_sem=send, recv_sem=recv,
            device_id={"neu": device(dq, dc)}, device_id_type=pl.DeviceIdType.MESH,
        )

    order = [1, 3, 2]
    order_w = [1, 3, 2]
    order_in = [1, 2, 3]
    order_out = [1, 3, 2]

    own = [
        pltpu.make_async_copy(wt_hbm, w_src, own_sem.at[0]),
        pltpu.make_async_copy(idx_hbm, i_src, own_sem.at[1]),
    ]
    loads = []
    for d in order + [0]:
        t = (q + d) % group
        cols = pl.ds(pl.multiple_of(t * lanes, lanes), lanes)
        a = pltpu.make_async_copy(val_hbm.at[:, cols], val.at[d], load_sem.at[0, d])
        b = pltpu.make_async_copy(mask_hbm.at[:, cols], mask.at[d], load_sem.at[1, d])
        loads.append((d, a, b))
    for a in own:
        a.start()
    for d, a, b in loads:
        a.start()
        b.start()

    partners = set()
    for dq in range(group):
        for s in shift:
            partners |= {(dq, s % classes), (dq, -s % classes)}
    for dc in range(classes):
        partners.add((0, dc))
    partners.discard((0, 0))
    barrier = pltpu.get_barrier_semaphore()
    for dq, dc in sorted(partners, reverse=True):
        pl.semaphore_signal(
            barrier, inc=1, device_id={"neu": device(dq, dc)},
            device_id_type=pl.DeviceIdType.MESH,
        )
    if pairs:
        x_me = lax.axis_index("img")
        half = x_me % 2
        twin = x_me + 1 - 2 * half
        share_rows = KB * IB // 2
        w_rows = pl.ds(pl.multiple_of(half * share_rows, share_rows), share_rows)
        pl.semaphore_signal(
            barrier, inc=1, device_id={"img": twin}, device_id_type=pl.DeviceIdType.MESH
        )
    else:
        w_rows = pl.ds(0, KB * IB)

    for d, a, b in loads:
        a.wait()
        b.wait()
        masked = (val[d].astype(jnp.float32) * mask[d].astype(jnp.float32))
        if d:
            y0[d] = masked.astype(jnp.bfloat16)
        else:
            ya[pl.ds(q * run_blocks, run_blocks)] = masked.reshape(run_blocks, IB, lanes)
    for a in own:
        a.wait()
    pl.semaphore_wait(barrier, len(partners) + (1 if pairs else 0))

    waits = []
    index_waits = [[] for _ in range(layers)]
    weight_sends = []
    weight_waits = [[] for _ in range(layers)]
    for l in range(layers):
        for dq in order_w + [0]:
            if dq == 0 and shift[l] % classes == 0:
                a = pltpu.make_async_copy(w_src.at[l], wt.at[l, q], w_recv.at[l, 0])
                b = pltpu.make_async_copy(i_src.at[l], idx_v.at[l, q], i_recv.at[l, 0])
                a.start()
                b.start()
                weight_waits[l].append(a.wait)
                index_waits[l].append(b.wait)
                continue
            b = remote(i_src.at[l], idx_v.at[l, q], i_send.at[l, dq], i_recv.at[l, dq], dq, shift[l])
            a = remote(
                w_src.at[l, w_rows], wt.at[l, q, w_rows], w_send.at[l, dq], w_recv.at[l, dq], dq, shift[l]
            )
            b.start()
            a.start()
            waits.extend([a.wait_send, b.wait_send])
            index_waits[l].append(b.wait_recv)
            weight_sends.append((l, dq, a))

    inputs = []
    for d in order_in:
        x = remote(y0.at[d], xin.at[d], in_send.at[d], in_recv.at[d], d, 0)
        x.start()
        waits.append(x.wait_send)
        inputs.append((d, x))

    for l, dq, a in weight_sends:
        a.wait_recv()
        if pairs:
            here = wt.at[l, (q + group - dq) % group, w_rows]
            x = pltpu.make_async_remote_copy(
                src_ref=here, dst_ref=here, send_sem=f_send.at[l, dq], recv_sem=f_recv.at[l, dq],
                device_id={"img": twin}, device_id_type=pl.DeviceIdType.MESH,
            )
            x.start()
            waits.append(x.wait_send)
            weight_waits[l].append(x.wait_recv)

    index_copies = []
    for l in range(layers):
        for w in index_waits[l]:
            w()
        x = pltpu.make_async_copy(idx_v.at[l], idx_s.at[l], s_sem.at[l])
        x.start()
        index_copies.append(x)

    per = min(4, blocks)
    width = per * OB
    m_of = lax.broadcasted_iota(jnp.int32, (width, width), 0) // (KB * IB)
    n_of = lax.broadcasted_iota(jnp.int32, (width, width), 1) // OB

    def prepare(l):
        for w in weight_waits[l]:
            w()
        for t in range(group):
            for g in range(blocks // per):
                w = wt[l, t, :, g * width:(g + 1) * width].astype(jnp.float32)
                wide = jnp.where(m_of == n_of, jnp.concatenate([w] * per, axis=0), 0.0)
                wd[l, t, g] = wide.T.astype(jnp.bfloat16)

    def advance(l, src, t):
        out = []
        for g in range(blocks // per):
            pieces = []
            for j in range(g * per, (g + 1) * per):
                for k in range(KB):
                    b = idx_s[l, t, k, j]
                    pieces.append(src[quotient(b, run_blocks * classes) * run_blocks + remainder(b, run_blocks)])
            picked = jnp.concatenate(pieces, axis=0).astype(jnp.bfloat16)
            summed = jnp.dot(wd[l, t, g], picked, preferred_element_type=jnp.float32)
            clamped = jnp.minimum(jnp.maximum(summed - bias_value, 0.0), ceiling)
            out.append(clamped.astype(jnp.bfloat16))
        return out

    for l in range(layers):
        prepare(l)
    for x in index_copies:
        x.wait()
    for d, x in inputs:
        x.wait_recv()
        s = (q + group - d) % group
        ya[pl.ds(s * run_blocks, run_blocks)] = xin[d].astype(jnp.float32).reshape(run_blocks, IB, lanes)

    src, dst = ya, yb
    for l in range(layers - 1):
        for t in range(group):
            for g, y in enumerate(advance(l, src, t)):
                first = t * run_blocks + g * width // IB
                dst[first:first + width // IB] = y.astype(jnp.float32).reshape(width // IB, IB, lanes)
        src, dst = dst, src

    total = jnp.zeros((8, lanes), jnp.float32)
    last = layers - 1
    outputs = []
    for d in order_out + [0]:
        t = (q + d) % group
        for g, y in enumerate(advance(last, src, t)):
            tiles[d, g * width:(g + 1) * width, :] = y
            total = total + jnp.sum(y.astype(jnp.float32).reshape(width // 8, 8, lanes), axis=0)
        x = remote(
            tiles.at[d], out_ref.at[:, pl.ds(pl.multiple_of(q * lanes, lanes), lanes)],
            o_send.at[d], o_recv.at[d], d, -shift[last],
        )
        x.start()
        waits.append(x.wait_send)
        outputs.append(x)

    part[...] = total
    sums = []
    for dc in range(1, classes):
        x = remote(part, parts.at[dc], r_send.at[dc], r_recv.at[dc], 0, dc)
        x.start()
        waits.append(x.wait_send)
        sums.append((dc, x))
    for dc, x in sums:
        x.wait_recv()
        total = total + parts[dc]
    row = jnp.sum(total, axis=0, keepdims=True)
    share = lanes // classes
    mine = jnp.zeros((1, share), jnp.float32)
    for j in range(classes):
        mine = jnp.where(c == j, row[:, j * share:(j + 1) * share], mine)
    rs_ref[...] = mine
    for x in outputs:
        x.wait_recv()
    for w in waits:
        w()


def on_device(classes, pairs, image_values, image_mask, weights, block_index):
    layers, rows = weights.shape[:2]
    blocks = block_index.shape[1]
    columns = image_values.shape[1]
    group = KB
    lanes = columns // group
    wt = jnp.transpose(weights, (0, 2, 3, 1)).reshape(layers, KB * IB, rows)
    idx = jnp.transpose(block_index, (0, 2, 1))
    per = min(4, blocks)
    bf16, f32, i32 = jnp.bfloat16, jnp.float32, jnp.int32
    V, S = pltpu.VMEM, pltpu.SMEM
    dma = pltpu.SemaphoreType.DMA
    any_spec = pl.BlockSpec(memory_space=pl.ANY)
    operands = [pltpu.with_memory_space_constraint(v, pltpu.HBM) for v in (image_values, image_mask, wt, idx)]
    out, sums = pl.pallas_call(
        functools.partial(kernel, (classes, pairs, layers, rows, blocks, lanes)),
        out_shape=(
            jax.ShapeDtypeStruct((rows, columns), bf16),
            jax.ShapeDtypeStruct((1, lanes // classes), f32),
        ),
        in_specs=[any_spec] * 4,
        out_specs=(pl.BlockSpec(memory_space=pltpu.VMEM), pl.BlockSpec(memory_space=pltpu.VMEM)),
        scratch_shapes=[
            V((group, rows, lanes), bf16),
            V((group, rows, lanes), i32),
            V((layers, KB * IB, rows), bf16),
            V((layers, KB, blocks), i32),
            V((group, rows, lanes), bf16),
            V((group, rows, lanes), bf16),
            V((group * rows // IB, IB, lanes), f32),
            V((group * rows // IB, IB, lanes), f32),
            V((layers, group, KB * IB, rows), bf16),
            V((layers, group, blocks // per, per * OB, per * KB * IB), bf16),
            V((layers, group, KB, blocks), i32),
            S((layers, group, KB, blocks), i32),
            V((group, rows, lanes), bf16),
            V((8, lanes), f32),
            V((classes, 8, lanes), f32),
            dma((2, group)), dma((2,)),
            dma((layers, group)), dma((layers, group)),
            dma((group,)), dma((group,)),
            dma((layers, group)), dma((layers, group)),
            dma((layers, group)), dma((layers, group)),
            dma((layers,)),
            dma((group,)), dma((group,)),
            dma((classes,)), dma((classes,)),
        ],
        compiler_params=pltpu.CompilerParams(collective_id=0, has_side_effects=True, vmem_limit_bytes=16 * 1024 * 1024),
    )(*operands)
    return out, sums.reshape(-1)


def solution(mesh):
    classes = mesh.shape["neu"] // KB
    in_specs = (P("neu", "img"), P("neu", "img"), P(None, "neu", None, None), P(None, "neu", None))
    out_specs = (P("neu", "img"), P(("img", "neu")))
    return jax.shard_map(
        functools.partial(on_device, classes, mesh.shape["img"] % 2 == 0), mesh=mesh, in_specs=in_specs,
        out_specs=out_specs, check_vma=False,
    )
```
